32 devices in a mesh: cuts: 2 (over y), blk: 4 (over z), sol: 4 (over x, core).
Axes of the slice: x: 2, y: 2, z: 4, core: 2. Of those that a mesh axis runs over, the one named last changes fastest.
Arguments:
- solutions: bfloat16 [20, 2, 3, 256, 4096], P('cuts', None, None, None, ('blk', 'sol')), parts along dimension 0, may hold values from -6 to 6
- eigvecs: bfloat16 [20, 2, 3, 128, 4096], P('cuts', None, None, None, ('blk', 'sol')), parts along dimension 0, may hold values from -430 to 430
Outputs:
- projected: float32 [128, 20, 2, 256], P(('blk', 'sol'), 'cuts'), parts along dimension 1
The draws below stay inside these ranges and needn't reach their ends.
There are 2 independent parts, one for each index of `cuts`. The reference program is written for one: setup_inputs(seed, part) draws one part's arguments, and reference() takes and returns one part's arrays. A program takes and returns all parts, laid end to end along the dimension named above; each array names one. Nothing has to cross between parts.
All inputs are finite; a program needn't handle non-finite values.
Results may differ from the reference program's by a relative error of at most 0.0003.
Values sent between devices are 32-bit elements; how exact they have to be, the bound alone decides.
A program may use at most 64 MiB of HBM per device.

```python
import math
import jax
import jax.numpy as jnp
from jax import lax

TS = 10
K = 128
COLORS = 3
NCOL = 256
SITES = 4096


def draw_eigvecs(key, part):
    key_base = jax.random.fold_in(key, 11)
    key_gain = jax.random.fold_in(key, 12)
    key_phase = jax.random.fold_in(key, 13)
    shape = (TS, 2, COLORS, K, SITES)
    base = jax.random.truncated_normal(key_base, -6.0, 6.0, shape, jnp.float32)
    scale = jnp.ones((TS, 1, 1, K, 1), jnp.float32)
    gains = jax.random.uniform(key_gain, (TS, 1, 1, K, 1), jnp.float32, 0.5, 1.5)
    phases = jax.random.uniform(key_phase, (TS, 1, 1, K, 1), jnp.float32, 0.0, 2.0 * math.pi)
    position = jnp.arange(SITES, dtype=jnp.float32) / SITES
    envelope = jnp.exp(gains * jnp.cos(2.0 * math.pi * position + phases))
    return (base * envelope * scale).astype(jnp.bfloat16)


def levels(rng, shape, pieces, least, top_value):
    factor_of, own = 1.0, jax.random.fold_in(rng, 6)
    for axis_at, shards_of in pieces:
        heights = jnp.exp(jax.random.uniform(jax.random.fold_in(own, axis_at), (shards_of,), jnp.float32, least / len(pieces), top_value / len(pieces)))
        factor_of = factor_of * jnp.repeat(heights, shape[axis_at] // shards_of).reshape([-1 if axis == axis_at else 1 for axis in range(len(shape))])
    return factor_of


def gaussian(own_key, extent, width, bound, cuts=(), held_as=jnp.bfloat16):
    entries = jax.random.normal(own_key, extent, jnp.float32) * width
    if len(cuts) > 0:
        entries = levels(own_key, extent, cuts, -0.22, 0.18) * entries
    return jnp.clip(entries, min=-bound, max=bound).astype(held_as)


def setup_inputs(seed: int = 0, part: int = 0) -> dict:
    streams_of = jax.random.split(jax.random.key(seed), 3)
    part_splits = jax.random.split(jax.random.fold_in(streams_of[2], part), 3)
    return {
        "solutions": gaussian(part_splits[0], (TS, 2, COLORS, NCOL, SITES), 1.0, 6.0, ((4, 16),)),
        "eigvecs": draw_eigvecs(jax.random.fold_in(jax.random.fold_in(streams_of[2], part), 71), part),
    }


def one_slice(pair):
    vectors, fields = pair
    vf = vectors.astype(jnp.float32)
    sf = fields.astype(jnp.float32)
    hi = lax.Precision.HIGHEST
    real = jnp.einsum('rckx,rcnx->kn', vf, sf, precision=hi)
    imag = jnp.einsum('ckx,cnx->kn', vf[0], sf[1], precision=hi) - jnp.einsum('ckx,cnx->kn', vf[1], sf[0], precision=hi)
    sumsq = lax.optimization_barrier(jnp.sum(vf * vf, axis=(0, 1, 3)))
    scale = lax.rsqrt(jnp.maximum(sumsq, jnp.float32(SITES)))
    return jnp.stack((real, imag), axis=1) * scale[:, None, None]

def reference(solutions, eigvecs):
    result = lax.map(one_slice, (eigvecs, solutions))
    return jnp.transpose(result, (1, 0, 2, 3))
```

```python
import functools

import jax
import jax.numpy as jnp
from jax import lax
from jax.experimental import pallas as pl
from jax.experimental.pallas import tpu as pltpu
from jax.sharding import PartitionSpec as P

MESH = pl.DeviceIdType.MESH
LANES = 128
SUBLANES = 8


def project_kernel(sizes, s_hbm, e_hbm, out, ev, sv, part, got1, got2, got3, nrm, ngot1, ngot2, ngot3,
                   in_sem, snd1, rcv1, snd2, rcv2, snd3, rcv3, nsnd1, nrcv1, nsnd2, nrcv2, nsnd3, nrcv3):
    slices, colors, rows, cols, chips_x, chips_z, own, floor_value = sizes
    blk = lax.axis_index("blk")
    sol = lax.axis_index("sol")
    core = lax.rem(sol, 2)
    x = sol // 2
    other = 1 - core
    partner = x * 2 + other

    def x_at(d):
        return lax.rem(x + d, chips_x)

    def z_at(d):
        return lax.rem(blk + d, chips_z)

    def x_dev(d):
        return {"sol": x_at(d) * 2 + core}

    def z_dev(d):
        return {"blk": z_at(d)}

    barrier = pltpu.get_barrier_semaphore()
    pl.semaphore_signal(barrier, inc=1, device_id={"sol": partner}, device_id_type=MESH)
    for d in range(1, chips_x):
        pl.semaphore_signal(barrier, inc=1, device_id=x_dev(d), device_id_type=MESH)
    for d in range(1, chips_z):
        pl.semaphore_signal(barrier, inc=1, device_id=z_dev(d), device_id_type=MESH)

    def in_e(t):
        return pltpu.make_async_copy(e_hbm.at[t], ev.at[t], in_sem.at[0, t])

    def in_s(t):
        return pltpu.make_async_copy(s_hbm.at[t], sv.at[t], in_sem.at[1, t])

    def remote(src, dst, a, b, dev):
        return pltpu.make_async_remote_copy(
            src_ref=src, dst_ref=dst, send_sem=a, recv_sem=b, device_id=dev, device_id_type=MESH
        )

    def copy1(t):
        return remote(part.at[t, other], got1.at[t], snd1.at[t], rcv1.at[t], {"sol": partner})

    def copy2(t, d):
        return remote(part.at[t, core, x_at(d)], got2.at[t, d - 1], snd2.at[t, d - 1], rcv2.at[t, d - 1], x_dev(d))

    def copy3(t, d):
        return remote(part.at[t, core, x, z_at(d)], got3.at[t, d - 1], snd3.at[t, d - 1], rcv3.at[t, d - 1], z_dev(d))

    ncopy1 = remote(nrm.at[other], ngot1, nsnd1, nrcv1, {"sol": partner})

    def ncopy2(d):
        return remote(nrm.at[core, x_at(d)], ngot2.at[d - 1], nsnd2.at[d - 1], nrcv2.at[d - 1], x_dev(d))

    def ncopy3(d):
        return remote(nrm.at[core, x, z_at(d)], ngot3.at[d - 1], nsnd3.at[d - 1], nrcv3.at[d - 1], z_dev(d))

    def start_in(t, _):
        in_e(t).start()
        in_s(t).start()
        return 0

    lax.fori_loop(0, slices, start_in, 0)
    nrm[...] = jnp.zeros_like(nrm)

    def compute(t):
        in_e(t).wait()
        in_s(t).wait()
        total = None
        squares = None
        for c in range(colors):
            a = ev[t, :, c]
            b = sv[t, :, c]
            a = a.reshape(2 * rows, a.shape[-1])
            b = b.reshape(2 * cols, b.shape[-1])
            p = lax.dot_general(a, b, (((1,), (1,)), ((), ())), preferred_element_type=jnp.float32)
            total = p if total is None else total + p
            wide = a.astype(jnp.float32)
            wide = wide * wide
            squares = wide if squares is None else squares + wide
        real = total[:rows, :cols] + total[rows:, cols:]
        imag = total[:rows, cols:] - total[rows:, :cols]
        real = real.reshape(chips_z, chips_x, 2, own, cols)
        imag = imag.reshape(chips_z, chips_x, 2, own, cols)
        squares = jnp.sum(squares[:rows] + squares[rows:], axis=1, keepdims=True)
        lane = lax.broadcasted_iota(jnp.int32, (rows, LANES), 1)
        mark = jnp.where(lane == t, squares, 0.0).reshape(chips_z, chips_x, 2, own, LANES)
        for k in range(2):
            for i in range(chips_x):
                part[t, k, i, :, :, :cols] = real[:, i, k]
                part[t, k, i, :, :, cols:] = imag[:, i, k]
                nrm[k, i] += mark[:, i, k]

    def after1(t):
        copy1(t).wait_recv()
        part[t, core] += got1[t]
        for d in range(1, chips_x):
            copy2(t, d).start()

    def after2(t):
        for d in range(1, chips_x):
            copy2(t, d).wait_recv()
        part[t, core, x] += jnp.sum(got2[t], axis=0)
        for d in range(1, chips_z):
            copy3(t, d).start()

    compute(0)
    pl.semaphore_wait(barrier, 1 + (chips_x - 1) + (chips_z - 1))
    copy1(0).start()

    lag1, lag2 = 1, 3

    def step(s, _):
        compute(s)
        copy1(s).start()

        @pl.when(s >= lag1)
        def _():
            after1(s - lag1)

        @pl.when(s >= lag2)
        def _():
            after2(s - lag2)

        return 0

    lax.fori_loop(1, slices, step, 0)
    ncopy1.start()
    for t in range(max(slices - lag1, 0), slices):
        after1(t)
    ncopy1.wait_recv()
    nrm[core] += ngot1[...]
    for d in range(1, chips_x):
        ncopy2(d).start()
    for t in range(max(slices - lag2, 0), slices):
        after2(t)
    for d in range(1, chips_x):
        ncopy2(d).wait_recv()
    nrm[core, x] += jnp.sum(ngot2[...], axis=0)
    for d in range(1, chips_z):
        ncopy3(d).start()
    for d in range(1, chips_z):
        ncopy3(d).wait_recv()
    sums = nrm[core, x, blk] + jnp.sum(ngot3[...], axis=0)
    scale = lax.rsqrt(jnp.maximum(sums, jnp.float32(floor_value)))
    for t in range(slices):
        for d in range(1, chips_z):
            copy3(t, d).wait_recv()
        done = (part[t, core, x, blk] + jnp.sum(got3[t], axis=0)) * scale[:, t : t + 1]
        out[:, t, 0, :] = done[:, :cols]
        out[:, t, 1, :] = done[:, cols:]

    def drain(t, _):
        copy1(t).wait_send()
        for d in range(1, chips_x):
            copy2(t, d).wait_send()
        for d in range(1, chips_z):
            copy3(t, d).wait_send()
        return 0

    lax.fori_loop(0, slices, drain, 0)
    ncopy1.wait_send()
    for d in range(1, chips_x):
        ncopy2(d).wait_send()
    for d in range(1, chips_z):
        ncopy3(d).wait_send()


def kernel_shards(chips_x, chips_z, solutions, eigvecs):
    slices, parts, colors, rows, local = eigvecs.shape
    cols = solutions.shape[3]
    own = rows // (chips_x * 2 * chips_z)
    sizes = (slices, colors, rows, cols, chips_x, chips_z, own, local * chips_x * 2 * chips_z)
    f32 = jnp.float32
    dma = pltpu.SemaphoreType.DMA
    wide = 2 * cols
    return pl.pallas_call(
        functools.partial(project_kernel, sizes),
        out_shape=jax.ShapeDtypeStruct((own, slices, 2, cols), f32),
        in_specs=[pl.BlockSpec(memory_space=pl.ANY)] * 2,
        out_specs=pl.BlockSpec(memory_space=pltpu.VMEM),
        scratch_shapes=[
            pltpu.VMEM(eigvecs.shape, eigvecs.dtype),
            pltpu.VMEM(solutions.shape, solutions.dtype),
            pltpu.VMEM((slices, 2, chips_x, chips_z, own, wide), f32),
            pltpu.VMEM((slices, chips_x, chips_z, own, wide), f32),
            pltpu.VMEM((slices, chips_x - 1, chips_z, own, wide), f32),
            pltpu.VMEM((slices, chips_z - 1, own, wide), f32),
            pltpu.VMEM((2, chips_x, chips_z, own, LANES), f32),
            pltpu.VMEM((chips_x, chips_z, own, LANES), f32),
            pltpu.VMEM((chips_x - 1, chips_z, own, LANES), f32),
            pltpu.VMEM((chips_z - 1, own, LANES), f32),
            dma((2, slices)),
            dma((slices,)), dma((slices,)),
            dma((slices, chips_x - 1)), dma((slices, chips_x - 1)),
            dma((slices, chips_z - 1)), dma((slices, chips_z - 1)),
            dma, dma,
            dma((chips_x - 1,)), dma((chips_x - 1,)),
            dma((chips_z - 1,)), dma((chips_z - 1,)),
        ],
        compiler_params=pltpu.CompilerParams(
            collective_id=0, has_side_effects=True, vmem_limit_bytes=60 * 1024 * 1024
        ),
    )(solutions, eigvecs)


def plain_shards(solutions, eigvecs):
    blocks = lax.axis_size("blk")
    within = lax.axis_size("sol")
    slices, _, _, total_rows, local_sites = eigvecs.shape
    sumsq = jnp.sum(jnp.square(eigvecs.astype(jnp.float32)), axis=(1, 2, 4))
    totals = lax.psum(sumsq, ("blk", "sol"))
    floor_value = jnp.float32(local_sites * blocks * within)
    scale = lax.rsqrt(jnp.maximum(totals, floor_value))
    own_rows = total_rows // (blocks * within)
    real = jnp.einsum("trckx,trcnx->ktn", eigvecs, solutions, preferred_element_type=jnp.float32)
    imag = jnp.einsum(
        "tckx,tcnx->ktn", eigvecs[:, 0], solutions[:, 1], preferred_element_type=jnp.float32
    )
    imag = imag - jnp.einsum(
        "tckx,tcnx->ktn", eigvecs[:, 1], solutions[:, 0], preferred_element_type=jnp.float32
    )
    summed = lax.psum_scatter(
        jnp.stack((real, imag), axis=2), ("blk", "sol"), scatter_dimension=0, tiled=True
    )
    owner = lax.axis_index("blk") * within + lax.axis_index("sol")
    mine = lax.dynamic_slice_in_dim(scale, owner * own_rows, own_rows, 1)
    return summed * jnp.transpose(mine)[:, :, None, None]


def solution(mesh):
    blocks, within = mesh.shape["blk"], mesh.shape["sol"]

    def shards(solutions, eigvecs):
        slices, rows = eigvecs.shape[0], eigvecs.shape[3]
        own = rows // (blocks * within)
        if own % SUBLANES or within % 2 or within < 4 or blocks < 2 or slices > LANES:
            return plain_shards(solutions, eigvecs)
        return kernel_shards(within // 2, blocks, solutions, eigvecs)

    in_specs = (
        P("cuts", None, None, None, ("blk", "sol")),
        P("cuts", None, None, None, ("blk", "sol")),
    )
    out_specs = P(("blk", "sol"), "cuts", None, None)
    return jax.shard_map(shards, mesh=mesh, in_specs=in_specs, out_specs=out_specs, check_vma=False)
```

```python
import functools

import jax
import jax.numpy as jnp
from jax import lax
from jax.experimental import pallas as pl
from jax.experimental.pallas import tpu as pltpu
from jax.sharding import PartitionSpec as P

MESH = pl.DeviceIdType.MESH
LANES = 128
SUBLANES = 8
EARLY_B = 3
LAG = 3
LAG2 = 1


def plan_of(slices):
    early = 2 * EARLY_B
    return "".join("B" if t < early and t % 2 else "A" for t in range(slices - 1)) + "D"


def project_kernel(sizes, s_hbm, e_hbm, out, ev, sv, part, got1, gotx, gotl, goth, gotbl, gotbx, gotd, nrm, ngot1, ngot2, ngot3,
                   in_sem, snd1, rcv1, sndx, rcvx, sndl, rcvl, sndh, rcvh, sndd, rcvd,
                   nsnd1, nrcv1, nsnd2, nrcv2, nsnd3, nrcv3):
    slices, colors, rows, cols, chips_x, chips_z, own, floor_value = sizes
    plan = plan_of(slices)
    high = chips_z // 2
    blk = lax.axis_index("blk")
    sol = lax.axis_index("sol")
    core = lax.rem(sol, 2)
    x = sol // 2
    l = lax.rem(blk, 2)
    h = blk // 2
    other = 1 - core
    partner = {"sol": x * 2 + other}
    beside = {"blk": h * 2 + 1 - l}

    def x_at(d):
        return lax.rem(x + d, chips_x)

    def h_at(d):
        return lax.rem(h + d, high)

    def z_at(d):
        return lax.rem(blk + d, chips_z)

    def x_dev(d):
        return {"sol": x_at(d) * 2 + core}

    def h_dev(d):
        return {"blk": h_at(d) * 2 + l}

    def z_dev(d):
        return {"blk": z_at(d)}

    xs, hs, zs = range(1, chips_x), range(1, high), range(1, chips_z)

    barrier = pltpu.get_barrier_semaphore()
    pl.semaphore_signal(barrier, inc=1, device_id=partner, device_id_type=MESH)
    for d in xs:
        pl.semaphore_signal(barrier, inc=1, device_id=x_dev(d), device_id_type=MESH)
    for d in zs:
        pl.semaphore_signal(barrier, inc=1, device_id=z_dev(d), device_id_type=MESH)

    def in_e(t):
        return pltpu.make_async_copy(e_hbm.at[t], ev.at[t], in_sem.at[0, t])

    def in_s(t):
        return pltpu.make_async_copy(s_hbm.at[t], sv.at[t], in_sem.at[1, t])

    started = []

    def remote(src, dst, a, b, dev):
        return pltpu.make_async_remote_copy(
            src_ref=src, dst_ref=dst, send_sem=a, recv_sem=b, device_id=dev, device_id_type=MESH
        )

    def go(copies):
        for copy in copies:
            copy.start()
            started.append(copy)

    def arrive(copies):
        for copy in copies:
            copy.wait_recv()

    def core_copies(t):
        return [remote(part.at[t, other], got1.at[t], snd1.at[t], rcv1.at[t], partner)]

    def x_copies(t):
        if plan[t] == "B":
            slot = plan[:t].count("B")
            return [remote(part.at[t, core, x_at(d), l], gotbx.at[slot, d - 1], sndx.at[t, d - 1], rcvx.at[t, d - 1], x_dev(d)) for d in xs]
        return [remote(part.at[t, core, x_at(d)], gotx.at[t, d - 1], sndx.at[t, d - 1], rcvx.at[t, d - 1], x_dev(d)) for d in xs]

    def low_copies(t):
        if plan[t] == "B":
            slot = plan[:t].count("B")
            return [remote(part.at[t, core, :, 1 - l], gotbl.at[slot], sndl.at[t], rcvl.at[t], beside)]
        return [remote(part.at[t, core, x, 1 - l], gotl.at[t], sndl.at[t], rcvl.at[t], beside)]

    def high_copies(t):
        if plan[t] == "D":
            return [remote(part.at[t, core, x, lax.rem(z_at(d), 2), z_at(d) // 2], gotd.at[d - 1], sndd.at[d - 1], rcvd.at[d - 1], z_dev(d)) for d in zs]
        return [remote(part.at[t, core, x, l, h_at(d)], goth.at[t, d - 1], sndh.at[t, d - 1], rcvh.at[t, d - 1], h_dev(d)) for d in hs]

    ncopy1 = [remote(nrm.at[other], ngot1, nsnd1, nrcv1, partner)]
    ncopy2 = [remote(nrm.at[core, x_at(d)], ngot2.at[d - 1], nsnd2.at[d - 1], nrcv2.at[d - 1], x_dev(d)) for d in xs]
    ncopy3 = [remote(nrm.at[core, x, lax.rem(z_at(d), 2), z_at(d) // 2], ngot3.at[d - 1], nsnd3.at[d - 1], nrcv3.at[d - 1], z_dev(d)) for d in zs]

    def start_in(t, _):
        in_e(t).start()
        in_s(t).start()
        return 0

    lax.fori_loop(0, slices, start_in, 0)
    nrm[...] = jnp.zeros_like(nrm)

    def compute(t):
        in_e(t).wait()
        in_s(t).wait()
        total = None
        squares = None
        for c in range(colors):
            a = ev[t, :, c]
            b = sv[t, :, c]
            a = a.reshape(2 * rows, a.shape[-1])
            b = b.reshape(2 * cols, b.shape[-1])
            p = lax.dot_general(a, b, (((1,), (1,)), ((), ())), preferred_element_type=jnp.float32)
            total = p if total is None else total + p
            wide = a.astype(jnp.float32)
            wide = wide * wide
            squares = wide if squares is None else squares + wide
        real = total[:rows, :cols] + total[rows:, cols:]
        imag = total[:rows, cols:] - total[rows:, :cols]
        real = real.reshape(high, 2, chips_x, 2, own, cols)
        imag = imag.reshape(high, 2, chips_x, 2, own, cols)
        squares = jnp.sum(squares[:rows] + squares[rows:], axis=1, keepdims=True)
        lane = lax.broadcasted_iota(jnp.int32, (rows, LANES), 1)
        mark = jnp.where(lane == t, squares, 0.0).reshape(high, 2, chips_x, 2, own, LANES)
        for k in range(2):
            for i in range(chips_x):
                for j in range(2):
                    part[t, k, i, j, :, :, :cols] = real[:, j, i, k]
                    part[t, k, i, j, :, :, cols:] = imag[:, j, i, k]
                    nrm[k, i, j] += mark[:, j, i, k]

    def after_core(t):
        arrive(core_copies(t))
        part[t, core] += got1[t]
        go(low_copies(t) if plan[t] == "B" else x_copies(t))

    def after_first(t):
        if plan[t] == "B":
            arrive(low_copies(t))
            part[t, core, :, l] += gotbl[plan[:t].count("B")]
            go(x_copies(t))
        else:
            arrive(x_copies(t))
            part[t, core, x] += jnp.sum(gotx[t], axis=0)
            go(high_copies(t) if plan[t] == "D" else low_copies(t))

    def after_second(t):
        if plan[t] == "B":
            arrive(x_copies(t))
            part[t, core, x, l] += jnp.sum(gotbx[plan[:t].count("B")], axis=0)
            go(high_copies(t))
        elif plan[t] == "A":
            arrive(low_copies(t))
            part[t, core, x, l] += gotl[t]
            go(high_copies(t))

    last = slices - 1
    for t in range(slices):
        compute(t)
        if t == 0:
            pl.semaphore_wait(barrier, 1 + (chips_x - 1) + (chips_z - 1))
        if t == last:
            go(ncopy1)
        go(core_copies(t))
        if t >= 1:
            after_core(t - 1)
        if t >= LAG:
            after_first(t - LAG)
        if t >= LAG + LAG2:
            after_second(t - LAG - LAG2)
    arrive(ncopy1)
    nrm[core] += ngot1[...]
    go(ncopy2)
    after_core(last)
    for s in range(slices, slices + LAG + LAG2):
        if s == last + LAG:
            arrive(ncopy2)
            nrm[core, x] += jnp.sum(ngot2[...], axis=0)
            go(ncopy3)
        if 0 <= s - LAG < slices:
            after_first(s - LAG)
        if 0 <= s - LAG - LAG2 < slices:
            after_second(s - LAG - LAG2)
    arrive(ncopy3)
    sums = nrm[core, x, l, h] + jnp.sum(ngot3[...], axis=0)
    scale = lax.rsqrt(jnp.maximum(sums, jnp.float32(floor_value)))
    for t in range(slices):
        arrive(high_copies(t))
        extra = jnp.sum(gotd[...] if plan[t] == "D" else goth[t], axis=0)
        done = (part[t, core, x, l, h] + extra) * scale[:, t : t + 1]
        out[:, t, 0, :] = done[:, :cols]
        out[:, t, 1, :] = done[:, cols:]
    for copy in started:
        copy.wait_send()


def kernel_shards(chips_x, chips_z, solutions, eigvecs):
    slices, parts, colors, rows, local = eigvecs.shape
    cols = solutions.shape[3]
    own = rows // (chips_x * 2 * chips_z)
    high = chips_z // 2
    bees = max(plan_of(slices).count("B"), 1)
    sizes = (slices, colors, rows, cols, chips_x, chips_z, own, local * chips_x * 2 * chips_z)
    f32 = jnp.float32
    dma = pltpu.SemaphoreType.DMA
    wide = 2 * cols
    return pl.pallas_call(
        functools.partial(project_kernel, sizes),
        out_shape=jax.ShapeDtypeStruct((own, slices, 2, cols), f32),
        in_specs=[pl.BlockSpec(memory_space=pl.ANY)] * 2,
        out_specs=pl.BlockSpec(memory_space=pltpu.VMEM),
        scratch_shapes=[
            pltpu.VMEM(eigvecs.shape, eigvecs.dtype),
            pltpu.VMEM(solutions.shape, solutions.dtype),
            pltpu.VMEM((slices, 2, chips_x, 2, high, own, wide), f32),
            pltpu.VMEM((slices, chips_x, 2, high, own, wide), f32),
            pltpu.VMEM((slices, chips_x - 1, 2, high, own, wide), f32),
            pltpu.VMEM((slices, high, own, wide), f32),
            pltpu.VMEM((slices, high - 1, own, wide), f32),
            pltpu.VMEM((bees, chips_x, high, own, wide), f32),
            pltpu.VMEM((bees, chips_x - 1, high, own, wide), f32),
            pltpu.VMEM((chips_z - 1, own, wide), f32),
            pltpu.VMEM((2, chips_x, 2, high, own, LANES), f32),
            pltpu.VMEM((chips_x, 2, high, own, LANES), f32),
            pltpu.VMEM((chips_x - 1, 2, high, own, LANES), f32),
            pltpu.VMEM((chips_z - 1, own, LANES), f32),
            dma((2, slices)),
            dma((slices,)), dma((slices,)),
            dma((slices, chips_x - 1)), dma((slices, chips_x - 1)),
            dma((slices,)), dma((slices,)),
            dma((slices, high - 1)), dma((slices, high - 1)),
            dma((chips_z - 1,)), dma((chips_z - 1,)),
            dma, dma,
            dma((chips_x - 1,)), dma((chips_x - 1,)),
            dma((chips_z - 1,)), dma((chips_z - 1,)),
        ],
        compiler_params=pltpu.CompilerParams(
            collective_id=0, has_side_effects=True, vmem_limit_bytes=60 * 1024 * 1024
        ),
    )(solutions, eigvecs)


def plain_shards(solutions, eigvecs):
    blocks = lax.axis_size("blk")
    within = lax.axis_size("sol")
    slices, _, _, total_rows, local_sites = eigvecs.shape
    sumsq = jnp.sum(jnp.square(eigvecs.astype(jnp.float32)), axis=(1, 2, 4))
    totals = lax.psum(sumsq, ("blk", "sol"))
    floor_value = jnp.float32(local_sites * blocks * within)
    scale = lax.rsqrt(jnp.maximum(totals, floor_value))
    own_rows = total_rows // (blocks * within)
    real = jnp.einsum("trckx,trcnx->ktn", eigvecs, solutions, preferred_element_type=jnp.float32)
    imag = jnp.einsum(
        "tckx,tcnx->ktn", eigvecs[:, 0], solutions[:, 1], preferred_element_type=jnp.float32
    )
    imag = imag - jnp.einsum(
        "tckx,tcnx->ktn", eigvecs[:, 1], solutions[:, 0], preferred_element_type=jnp.float32
    )
    summed = lax.psum_scatter(
        jnp.stack((real, imag), axis=2), ("blk", "sol"), scatter_dimension=0, tiled=True
    )
    owner = lax.axis_index("blk") * within + lax.axis_index("sol")
    mine = lax.dynamic_slice_in_dim(scale, owner * own_rows, own_rows, 1)
    return summed * jnp.transpose(mine)[:, :, None, None]


def solution(mesh):
    blocks, within = mesh.shape["blk"], mesh.shape["sol"]

    def shards(solutions, eigvecs):
        slices, rows = eigvecs.shape[0], eigvecs.shape[3]
        own = rows // (blocks * within)
        if own % SUBLANES or within % 2 or within < 4 or blocks % 2 or blocks < 4 or slices < 2 or slices > LANES:
            return plain_shards(solutions, eigvecs)
        return kernel_shards(within // 2, blocks, solutions, eigvecs)

    in_specs = (
        P("cuts", None, None, None, ("blk", "sol")),
        P("cuts", None, None, None, ("blk", "sol")),
    )
    out_specs = P(("blk", "sol"), "cuts", None, None)
    return jax.shard_map(shards, mesh=mesh, in_specs=in_specs, out_specs=out_specs, check_vma=False)
```

```python
import functools

import jax
import jax.numpy as jnp
from jax import lax
from jax.experimental import pallas as pl
from jax.experimental.pallas import tpu as pltpu
from jax.sharding import PartitionSpec as P

MESH = pl.DeviceIdType.MESH
LANES = 128
SUBLANES = 8
EARLY_B = 3
LAG = 6
LAG2 = 4
AHEAD = 3


def plan_of(slices):
    early = 2 * EARLY_B
    return "".join("B" if t < early and t % 2 else "A" for t in range(slices - 1)) + "D"


def project_kernel(sizes, s_hbm, e_hbm, out, ev, sv, part, got1, gotx, gotl, goth, gotbl, gotbx, gotd, nrm, ngot1, ngot2, ngot3,
                   in_sem, snd1, rcv1, sndx, rcvx, sndl, rcvl, sndh, rcvh, sndd, rcvd,
                   nsnd1, nrcv1, nsnd2, nrcv2, nsnd3, nrcv3):
    slices, colors, rows, cols, chips_x, chips_z, own, floor_value = sizes
    plan = plan_of(slices)
    high = chips_z // 2
    blk = lax.axis_index("blk")
    sol = lax.axis_index("sol")
    core = lax.rem(sol, 2)
    x = sol // 2
    l = lax.rem(blk, 2)
    h = blk // 2
    other = 1 - core
    partner = {"sol": x * 2 + other}
    beside = {"blk": h * 2 + 1 - l}

    def x_at(d):
        return lax.rem(x + d, chips_x)

    def h_at(d):
        return lax.rem(h + d, high)

    def z_at(d):
        return lax.rem(blk + d, chips_z)

    def x_dev(d):
        return {"sol": x_at(d) * 2 + core}

    def h_dev(d):
        return {"blk": h_at(d) * 2 + l}

    def z_dev(d):
        return {"blk": z_at(d)}

    xs, hs, zs = range(1, chips_x), range(1, high), range(1, chips_z)

    barrier = pltpu.get_barrier_semaphore()
    pl.semaphore_signal(barrier, inc=1, device_id=partner, device_id_type=MESH)
    for d in xs:
        pl.semaphore_signal(barrier, inc=1, device_id=x_dev(d), device_id_type=MESH)
    for d in zs:
        pl.semaphore_signal(barrier, inc=1, device_id=z_dev(d), device_id_type=MESH)

    def in_e(t):
        return pltpu.make_async_copy(e_hbm.at[t], ev.at[t], in_sem.at[0, t])

    def in_s(t):
        return pltpu.make_async_copy(s_hbm.at[t], sv.at[t], in_sem.at[1, t])

    started = []

    def remote(src, dst, a, b, dev):
        return pltpu.make_async_remote_copy(
            src_ref=src, dst_ref=dst, send_sem=a, recv_sem=b, device_id=dev, device_id_type=MESH
        )

    def go(copies):
        for copy in copies:
            copy.start()
            started.append(copy)

    def arrive(copies):
        for copy in copies:
            copy.wait_recv()

    def core_copies(t):
        return [remote(part.at[t, other], got1.at[t], snd1.at[t], rcv1.at[t], partner)]

    def x_copies(t):
        if plan[t] == "B":
            slot = plan[:t].count("B")
            return [remote(part.at[t, core, x_at(d), l], gotbx.at[slot, d - 1], sndx.at[t, d - 1], rcvx.at[t, d - 1], x_dev(d)) for d in xs]
        return [remote(part.at[t, core, x_at(d)], gotx.at[t, d - 1], sndx.at[t, d - 1], rcvx.at[t, d - 1], x_dev(d)) for d in xs]

    def low_copies(t):
        if plan[t] == "B":
            slot = plan[:t].count("B")
            return [remote(part.at[t, core, :, 1 - l], gotbl.at[slot], sndl.at[t], rcvl.at[t], beside)]
        return [remote(part.at[t, core, x, 1 - l], gotl.at[t], sndl.at[t], rcvl.at[t], beside)]

    def high_copies(t):
        if plan[t] == "D":
            return [remote(part.at[t, core, x, lax.rem(z_at(d), 2), z_at(d) // 2], gotd.at[d - 1], sndd.at[d - 1], rcvd.at[d - 1], z_dev(d)) for d in zs]
        return [remote(part.at[t, core, x, l, h_at(d)], goth.at[t, d - 1], sndh.at[t, d - 1], rcvh.at[t, d - 1], h_dev(d)) for d in hs]

    ncopy1 = [remote(nrm.at[other], ngot1, nsnd1, nrcv1, partner)]
    ncopy2 = [remote(nrm.at[core, x_at(d)], ngot2.at[d - 1], nsnd2.at[d - 1], nrcv2.at[d - 1], x_dev(d)) for d in xs]
    ncopy3 = [remote(nrm.at[core, x, lax.rem(z_at(d), 2), z_at(d) // 2], ngot3.at[d - 1], nsnd3.at[d - 1], nrcv3.at[d - 1], z_dev(d)) for d in zs]

    def start_in(t):
        in_e(t).start()
        in_s(t).start()

    start_in(0)
    nrm[...] = jnp.zeros_like(nrm)

    def compute(t):
        in_e(t).wait()
        in_s(t).wait()
        for ahead in range(t + AHEAD if t else 1, min(t + AHEAD + 1, slices)):
            start_in(ahead)
        total = None
        squares = None
        for c in range(colors):
            a = ev[t, :, c]
            b = sv[t, :, c]
            a = a.reshape(2 * rows, a.shape[-1])
            b = b.reshape(2 * cols, b.shape[-1])
            p = lax.dot_general(a, b, (((1,), (1,)), ((), ())), preferred_element_type=jnp.float32)
            total = p if total is None else total + p
            wide = a.astype(jnp.float32)
            wide = wide * wide
            squares = wide if squares is None else squares + wide
        real = total[:rows, :cols] + total[rows:, cols:]
        imag = total[:rows, cols:] - total[rows:, :cols]
        real = real.reshape(high, 2, chips_x, 2, own, cols)
        imag = imag.reshape(high, 2, chips_x, 2, own, cols)
        squares = jnp.sum(squares[:rows] + squares[rows:], axis=1, keepdims=True)
        lane = lax.broadcasted_iota(jnp.int32, (rows, LANES), 1)
        mark = jnp.where(lane == t, squares, 0.0).reshape(high, 2, chips_x, 2, own, LANES)
        for k in range(2):
            for i in range(chips_x):
                for j in range(2):
                    part[t, k, i, j, :, :, :cols] = real[:, j, i, k]
                    part[t, k, i, j, :, :, cols:] = imag[:, j, i, k]
                    nrm[k, i, j] += mark[:, j, i, k]

    def after_core(t):
        arrive(core_copies(t))
        part[t, core] += got1[t]
        go(low_copies(t) if plan[t] == "B" else x_copies(t))

    def after_first(t):
        if plan[t] == "B":
            arrive(low_copies(t))
            part[t, core, :, l] += gotbl[plan[:t].count("B")]
            go(x_copies(t))
        else:
            arrive(x_copies(t))
            part[t, core, x] += jnp.sum(gotx[t], axis=0)
            go(high_copies(t) if plan[t] == "D" else low_copies(t))

    def after_second(t):
        if plan[t] == "B":
            arrive(x_copies(t))
            part[t, core, x, l] += jnp.sum(gotbx[plan[:t].count("B")], axis=0)
            go(high_copies(t))
        elif plan[t] == "A":
            arrive(low_copies(t))
            part[t, core, x, l] += gotl[t]
            go(high_copies(t))

    last = slices - 1
    for t in range(slices):
        compute(t)
        if t == 0:
            pl.semaphore_wait(barrier, 1 + (chips_x - 1) + (chips_z - 1))
        if t == last:
            go(ncopy1)
        go(core_copies(t))
        if t >= 1:
            after_core(t - 1)
        if t >= LAG:
            after_first(t - LAG)
        if t >= LAG + LAG2:
            after_second(t - LAG - LAG2)
    arrive(ncopy1)
    nrm[core] += ngot1[...]
    go(ncopy2)
    after_core(last)
    for s in range(slices, slices + LAG + LAG2):
        if s == last + LAG:
            arrive(ncopy2)
            nrm[core, x] += jnp.sum(ngot2[...], axis=0)
            go(ncopy3)
        if 0 <= s - LAG < slices:
            after_first(s - LAG)
        if 0 <= s - LAG - LAG2 < slices:
            after_second(s - LAG - LAG2)
    arrive(ncopy3)
    sums = nrm[core, x, l, h] + jnp.sum(ngot3[...], axis=0)
    scale = lax.rsqrt(jnp.maximum(sums, jnp.float32(floor_value)))
    for t in range(slices):
        arrive(high_copies(t))
        extra = jnp.sum(gotd[...] if plan[t] == "D" else goth[t], axis=0)
        done = (part[t, core, x, l, h] + extra) * scale[:, t : t + 1]
        out[:, t, 0, :] = done[:, :cols]
        out[:, t, 1, :] = done[:, cols:]
    for copy in started:
        copy.wait_send()


def kernel_shards(chips_x, chips_z, solutions, eigvecs):
    slices, parts, colors, rows, local = eigvecs.shape
    cols = solutions.shape[3]
    own = rows // (chips_x * 2 * chips_z)
    high = chips_z // 2
    bees = max(plan_of(slices).count("B"), 1)
    sizes = (slices, colors, rows, cols, chips_x, chips_z, own, local * chips_x * 2 * chips_z)
    f32 = jnp.float32
    dma = pltpu.SemaphoreType.DMA
    wide = 2 * cols
    return pl.pallas_call(
        functools.partial(project_kernel, sizes),
        out_shape=jax.ShapeDtypeStruct((own, slices, 2, cols), f32),
        in_specs=[pl.BlockSpec(memory_space=pl.ANY)] * 2,
        out_specs=pl.BlockSpec(memory_space=pltpu.VMEM),
        scratch_shapes=[
            pltpu.VMEM(eigvecs.shape, eigvecs.dtype),
            pltpu.VMEM(solutions.shape, solutions.dtype),
            pltpu.VMEM((slices, 2, chips_x, 2, high, own, wide), f32),
            pltpu.VMEM((slices, chips_x, 2, high, own, wide), f32),
            pltpu.VMEM((slices, chips_x - 1, 2, high, own, wide), f32),
            pltpu.VMEM((slices, high, own, wide), f32),
            pltpu.VMEM((slices, high - 1, own, wide), f32),
            pltpu.VMEM((bees, chips_x, high, own, wide), f32),
            pltpu.VMEM((bees, chips_x - 1, high, own, wide), f32),
            pltpu.VMEM((chips_z - 1, own, wide), f32),
            pltpu.VMEM((2, chips_x, 2, high, own, LANES), f32),
            pltpu.VMEM((chips_x, 2, high, own, LANES), f32),
            pltpu.VMEM((chips_x - 1, 2, high, own, LANES), f32),
            pltpu.VMEM((chips_z - 1, own, LANES), f32),
            dma((2, slices)),
            dma((slices,)), dma((slices,)),
            dma((slices, chips_x - 1)), dma((slices, chips_x - 1)),
            dma((slices,)), dma((slices,)),
            dma((slices, high - 1)), dma((slices, high - 1)),
            dma((chips_z - 1,)), dma((chips_z - 1,)),
            dma, dma,
            dma((chips_x - 1,)), dma((chips_x - 1,)),
            dma((chips_z - 1,)), dma((chips_z - 1,)),
        ],
        compiler_params=pltpu.CompilerParams(
            collective_id=0, has_side_effects=True, vmem_limit_bytes=52 * 1024 * 1024
        ),
    )(solutions, eigvecs)


def plain_shards(solutions, eigvecs):
    blocks = lax.axis_size("blk")
    within = lax.axis_size("sol")
    slices, _, _, total_rows, local_sites = eigvecs.shape
    sumsq = jnp.sum(jnp.square(eigvecs.astype(jnp.float32)), axis=(1, 2, 4))
    totals = lax.psum(sumsq, ("blk", "sol"))
    floor_value = jnp.float32(local_sites * blocks * within)
    scale = lax.rsqrt(jnp.maximum(totals, floor_value))
    own_rows = total_rows // (blocks * within)
    real = jnp.einsum("trckx,trcnx->ktn", eigvecs, solutions, preferred_element_type=jnp.float32)
    imag = jnp.einsum(
        "tckx,tcnx->ktn", eigvecs[:, 0], solutions[:, 1], preferred_element_type=jnp.float32
    )
    imag = imag - jnp.einsum(
        "tckx,tcnx->ktn", eigvecs[:, 1], solutions[:, 0], preferred_element_type=jnp.float32
    )
    summed = lax.psum_scatter(
        jnp.stack((real, imag), axis=2), ("blk", "sol"), scatter_dimension=0, tiled=True
    )
    owner = lax.axis_index("blk") * within + lax.axis_index("sol")
    mine = lax.dynamic_slice_in_dim(scale, owner * own_rows, own_rows, 1)
    return summed * jnp.transpose(mine)[:, :, None, None]


def solution(mesh):
    blocks, within = mesh.shape["blk"], mesh.shape["sol"]

    def shards(solutions, eigvecs):
        slices, rows = eigvecs.shape[0], eigvecs.shape[3]
        own = rows // (blocks * within)
        if own % SUBLANES or within % 2 or within < 4 or blocks % 2 or blocks < 4 or slices < 2 or slices > LANES:
            return plain_shards(solutions, eigvecs)
        return kernel_shards(within // 2, blocks, solutions, eigvecs)

    in_specs = (
        P("cuts", None, None, None, ("blk", "sol")),
        P("cuts", None, None, None, ("blk", "sol")),
    )
    out_specs = P(("blk", "sol"), "cuts", None, None)
    return jax.shard_map(shards, mesh=mesh, in_specs=in_specs, out_specs=out_specs, check_vma=False)
```
